32 devices in a mesh: dp: 8 (over z, core), tp: 4 (over y, x).
Axes of the slice: x: 2, y: 2, z: 4, core: 2. Of those that a mesh axis runs over, the one named last changes fastest.
Arguments:
- master: float32 [4096, 10240], P(('dp', 'tp')), may hold values from -0.09375 to 0.09375
- grad: float32 [4096, 10240], P(('dp', 'tp')), may hold values from -0.006 to 0.006
- exp_avg: float32 [4096, 10240], P(('dp', 'tp')), may hold values from -0.006 to 0.006
- exp_avg_sq: float32 [4096, 10240], P(('dp', 'tp')), may hold values from 1e-08 to 1e-05
Outputs:
- new_master: float32 [4096, 10240], P(('dp', 'tp'))
- new_avg: float32 [4096, 10240], P(('dp', 'tp'))
- new_avg_sq: float32 [4096, 10240], P(('dp', 'tp'))
- engine_qkv: bfloat16 [4096, 10240], P(None, 'tp')
The draws below stay inside these ranges and needn't reach their ends.
All inputs are finite; a program needn't handle non-finite values.
Results may differ from the reference program's by a relative error of at most 0.001.
Values may be sent and summed in bfloat16 or wider, within the bound.
A program may use at most 128 MiB of HBM per device.

```python
import math
import jax
import jax.numpy as jnp

QH = 64
KVH = 8
HS = 128
D_WIN = 4096
QKVW = 10240
N_TP = 4


def level_of(own_key, dims, pieces, smallest, top_value):
    def one(position, shards_of):
        heights = jax.random.uniform(jax.random.fold_in(jax.random.fold_in(own_key, 6), position), (shards_of,), jnp.float32, smallest / len(pieces), top_value / len(pieces))
        return jnp.repeat(jnp.exp(heights), dims[position] // shards_of).reshape((-1,) + (1,) * (len(dims) - position - 1))

    gain = one(*pieces[0])
    for cut in pieces[1:]:
        gain = gain * one(*cut)
    return gain


def scatter_about(rng, extent, width, most, shards=(), dtype=jnp.bfloat16):
    array = jax.random.normal(rng, extent, jnp.float32) * width
    if len(shards) > 0:
        array = level_of(rng, extent, shards, -0.22, 0.18) * array
    return jnp.clip(array, min=-most, max=most).astype(dtype)


def setup_inputs(seed: int = 0) -> dict:
    arg_keys = jax.random.split(jax.random.key(seed), 5)
    return {
        "master": scatter_about(arg_keys[0], (D_WIN, QKVW), D_WIN ** -0.5, 0.09375, ((0, 32),), jnp.float32),
        "grad": scatter_about(arg_keys[1], (D_WIN, QKVW), 0.001, 0.006, ((0, 32),), jnp.float32),
        "exp_avg": scatter_about(arg_keys[2], (D_WIN, QKVW), 0.001, 0.006, ((0, 32),), jnp.float32),
        "exp_avg_sq": jnp.clip(jnp.exp(math.log(9.999999747378752e-06) - 6.9077553 * jax.random.uniform(arg_keys[3], (D_WIN, QKVW), jnp.float32) ** level_of(arg_keys[3], (D_WIN, QKVW), ((0, 32),), -0.2, 0.2)), 9.99999993922529e-09, 9.999999747378752e-06),
    }


def joined_slices(weights, tp_count):
    rows = weights.shape[0]
    query = weights[:, :QH * HS].reshape(rows, tp_count, QH // tp_count * HS)
    keys = weights[:, QH * HS:(QH + KVH) * HS].reshape(rows, tp_count, KVH // tp_count * HS)
    values = weights[:, (QH + KVH) * HS:].reshape(rows, tp_count, KVH // tp_count * HS)
    return jnp.concatenate([query, keys, values], axis=2).reshape(rows, -1)

def reference(master, grad, exp_avg, exp_avg_sq):
    corr_one = 1.0 - 0.9 ** 10
    corr_two = 1.0 - 0.999 ** 10
    new_avg = 0.9 * exp_avg + 0.1 * grad
    new_avg_sq = 0.999 * exp_avg_sq + 0.001 * grad * grad
    update = new_avg / corr_one / (jnp.sqrt(new_avg_sq / corr_two) + 1e-08)
    new_master = master - 0.001 * (update + 0.1 * master)
    engine_qkv = joined_slices(new_master, N_TP).astype(jnp.bfloat16)
    return (new_master, new_avg, new_avg_sq, engine_qkv)
```

```python
import functools

import jax
import jax.numpy as jnp
from jax import lax
from jax.experimental import pallas as pl
from jax.experimental.pallas import tpu as pltpu
from jax.sharding import PartitionSpec as P

QH = 64
KVH = 8
HS = 128
CORES = 2
MESH = pl.DeviceIdType.MESH


def step_math(master, grad, exp_avg, exp_avg_sq):
    corr_one = 1.0 - 0.9**10
    corr_two = 1.0 - 0.999**10
    new_avg = 0.9 * exp_avg + 0.1 * grad
    new_avg_sq = 0.999 * exp_avg_sq + 0.001 * grad * grad
    update = new_avg / corr_one / (jnp.sqrt(new_avg_sq / corr_two) + 1e-08)
    new_master = master - 0.001 * (update + 0.1 * master)
    return new_master, new_avg, new_avg_sq


def pieces_of(tp_count):
    q, kv = QH // tp_count * HS, KVH // tp_count * HS
    return [
        [(t * q, q, 0), (QH * HS + t * kv, kv, q), ((QH + KVH) * HS + t * kv, kv, q + kv)]
        for t in range(tp_count)
    ]


def step_kernel(tp_count, m_ref, g_ref, a_ref, s_ref, nm_ref, na_ref, ns_ref, out_ref):
    for t, pieces in enumerate(pieces_of(tp_count)):
        for start, width, into in pieces:
            cols = pl.ds(start, width)
            new_master, new_avg, new_avg_sq = step_math(
                m_ref[:, cols], g_ref[:, cols], a_ref[:, cols], s_ref[:, cols]
            )
            nm_ref[:, cols] = new_master
            na_ref[:, cols] = new_avg
            ns_ref[:, cols] = new_avg_sq
            out_ref[t, :, pl.ds(into, width)] = new_master.astype(jnp.bfloat16)


def local_step(tp_count, master, grad, exp_avg, exp_avg_sq):
    rows, cols = master.shape
    tile = 16
    flat = pl.BlockSpec((tile, cols), lambda i: (i, 0))
    f32 = jax.ShapeDtypeStruct((rows, cols), jnp.float32)
    return pl.pallas_call(
        functools.partial(step_kernel, tp_count),
        grid=(rows // tile,),
        in_specs=[flat] * 4,
        out_specs=[flat] * 3 + [pl.BlockSpec((tp_count, tile, cols // tp_count), lambda i: (0, i, 0))],
        out_shape=[f32] * 3 + [jax.ShapeDtypeStruct((tp_count, rows, cols // tp_count), jnp.bfloat16)],
        compiler_params=pltpu.CompilerParams(vmem_limit_bytes=56 * 2**20),
        cost_estimate=pl.CostEstimate(flops=20 * rows * cols, bytes_accessed=30 * rows * cols, transcendentals=rows * cols),
    )(master, grad, exp_avg, exp_avg_sq)


def mix(t, j, count):
    out, bit = 0, 1
    while bit < count:
        out = out + ((t // bit) % 2 + (j // bit) % 2) % 2 * bit
        bit *= 2
    return out


def spread_kernel(dp_count, tp_count, parts, own_ref, out_ref, own_sem, flat_send, up_send, down_send, side_send, in_recv, side_recv):
    planes = dp_count // CORES
    dp, t = lax.axis_index("dp"), lax.axis_index("tp")
    z, core = dp // CORES, dp % CORES
    rows = own_ref.shape[1]
    part_rows = rows // parts
    has_up, has_down = z < planes - 1, z > 0
    units = tp_count * parts

    up = {"dp": dp + CORES}
    down = {"dp": dp - CORES}
    side = {"dp": z * CORES + 1 - core}

    barrier = pltpu.get_barrier_semaphore()
    for j in range(1, tp_count):
        pl.semaphore_signal(barrier, inc=1, device_id={"tp": mix(t, j, tp_count)}, device_id_type=MESH)
    pl.semaphore_signal(barrier, inc=1, device_id=side, device_id_type=MESH)

    @pl.when(has_up)
    def _():
        pl.semaphore_signal(barrier, inc=1, device_id=up, device_id_type=MESH)

    @pl.when(has_down)
    def _():
        pl.semaphore_signal(barrier, inc=1, device_id=down, device_id_type=MESH)

    pl.semaphore_wait(barrier, tp_count + has_up.astype(jnp.int32) + has_down.astype(jnp.int32))

    def place(plane, which_core, unit):
        source = mix(t, unit // parts, tp_count)
        block = (plane * CORES + which_core) * tp_count + source
        start = block * rows + unit % parts * part_rows
        return out_ref.at[pl.ds(pl.multiple_of(start, part_rows), part_rows), :]

    def copy(src, dst, send, recv, target):
        return pltpu.make_async_remote_copy(
            src_ref=src, dst_ref=dst, send_sem=send, recv_sem=recv, device_id=target, device_id_type=MESH
        )

    def going_up(src, plane, unit):
        return copy(src, place(plane, core, unit), up_send.at[plane, unit], in_recv.at[plane, unit], up)

    def going_down(src, plane, unit):
        return copy(src, place(plane, core, unit), down_send.at[plane, unit], in_recv.at[plane, unit], down)

    def going_side(src, plane, unit):
        return copy(src, place(plane, core, unit), side_send.at[plane, unit], side_recv.at[plane, unit], side)

    def arrived(plane, unit):
        here = place(plane, core, unit)
        copy(here, here, side_send.at[plane, unit], in_recv.at[plane, unit], side).wait_recv()

    def own_part(which, h):
        return own_ref.at[which, pl.ds(h * part_rows, part_rows), :]

    def flat_copy(j, h):
        target = mix(t, j, tp_count)
        start = ((z * CORES + core) * tp_count + t) * rows + h * part_rows
        dst = out_ref.at[pl.ds(pl.multiple_of(start, part_rows), part_rows), :]
        unit = j * parts + h
        return copy(own_part(target, h), dst, flat_send.at[unit], in_recv.at[z, unit], {"tp": target})

    def onward(src, unit):
        @pl.when(has_up)
        def _():
            going_up(src, z, unit).start()

        @pl.when(has_down)
        def _():
            going_down(src, z, unit).start()

    for h in range(parts):
        onward(own_part(t, h), h)
    for j in range(1, tp_count):
        for h in range(parts):
            flat_copy(j, h).start()
    keep = [pltpu.make_async_copy(own_part(t, h), place(z, core, h), own_sem.at[h]) for h in range(parts)]
    for h in range(parts):
        keep[h].start()
        going_side(own_part(t, h), z, h).start()

    @pl.loop(parts, units)
    def _(unit):
        arrived(z, unit)
        onward(place(z, core, unit), unit)
        going_side(place(z, core, unit), z, unit).start()

    @pl.loop(0, (planes - 1) * units)
    def _(m):
        distance, unit = m // units + 1, m % units
        below, above = z - distance, z + distance

        @pl.when(below >= 0)
        def _():
            arrived(below, unit)

            @pl.when(has_up)
            def _():
                going_up(place(below, core, unit), below, unit).start()

            going_side(place(below, core, unit), below, unit).start()

        @pl.when(above < planes)
        def _():
            arrived(above, unit)

            @pl.when(has_down)
            def _():
                going_down(place(above, core, unit), above, unit).start()

            going_side(place(above, core, unit), above, unit).start()

    for h in range(parts):
        keep[h].wait()
    for j in range(1, tp_count):
        for h in range(parts):
            flat_copy(j, h).wait_send()

    @pl.loop(0, planes * units)
    def _(m):
        plane, unit = m // units, m % units
        here = place(plane, core, unit)
        there = place(plane, 1 - core, unit)

        @pl.when((plane <= z) & has_up)
        def _():
            going_up(here, plane, unit).wait_send()

        @pl.when((plane >= z) & has_down)
        def _():
            going_down(here, plane, unit).wait_send()

        going_side(here, plane, unit).wait_send()
        copy(there, there, side_send.at[plane, unit], side_recv.at[plane, unit], side).wait_recv()


def spread(dp_count, tp_count, own):
    rows, width = own.shape[1:]
    parts = 2 if rows % 64 == 0 else 1
    planes, units = dp_count // CORES, tp_count * parts
    grid = pltpu.SemaphoreType.DMA((planes, units))
    return pl.pallas_call(
        functools.partial(spread_kernel, dp_count, tp_count, parts),
        in_specs=[pl.BlockSpec(memory_space=SRC)],
        out_specs=pl.BlockSpec(memory_space=DST),
        out_shape=jax.ShapeDtypeStruct((dp_count * tp_count * rows, width), jnp.bfloat16),
        scratch_shapes=[pltpu.SemaphoreType.DMA((parts,)), pltpu.SemaphoreType.DMA((units,))] + [grid] * 5,
        compiler_params=pltpu.CompilerParams(collective_id=0, has_side_effects=True, vmem_limit_bytes=LIMIT),
        cost_estimate=pl.CostEstimate(flops=0, bytes_accessed=2 * dp_count * tp_count * rows * width, transcendentals=0),
    )(own)


SRC = pl.ANY
DST = pl.ANY
LIMIT = 4 * 2**20


def body(dp_count, tp_count, master, grad, exp_avg, exp_avg_sq):
    new_master, new_avg, new_avg_sq, own = local_step(tp_count, master, grad, exp_avg, exp_avg_sq)
    return new_master, new_avg, new_avg_sq, spread(dp_count, tp_count, own)


def solution(mesh):
    flat = P(("dp", "tp"), None)
    return jax.shard_map(
        functools.partial(body, mesh.shape["dp"], mesh.shape["tp"]),
        mesh=mesh,
        in_specs=(flat,) * 4,
        out_specs=(flat, flat, flat, P(None, "tp")),
        check_vma=False,
    )
```

```python
import functools

import jax
import jax.numpy as jnp
from jax import lax
from jax.experimental import pallas as pl
from jax.experimental.pallas import tpu as pltpu
from jax.sharding import PartitionSpec as P

QH = 64
KVH = 8
HS = 128
CORES = 2
MESH = pl.DeviceIdType.MESH


def step_math(master, grad, exp_avg, exp_avg_sq):
    corr_one = 1.0 - 0.9**10
    corr_two = 1.0 - 0.999**10
    new_avg = 0.9 * exp_avg + 0.1 * grad
    new_avg_sq = 0.999 * exp_avg_sq + 0.001 * grad * grad
    update = new_avg / corr_one / (jnp.sqrt(new_avg_sq / corr_two) + 1e-08)
    new_master = master - 0.001 * (update + 0.1 * master)
    return new_master, new_avg, new_avg_sq


def pieces_of(tp_count):
    q, kv = QH // tp_count * HS, KVH // tp_count * HS
    return [
        [(t * q, q, 0), (QH * HS + t * kv, kv, q), ((QH + KVH) * HS + t * kv, kv, q + kv)]
        for t in range(tp_count)
    ]


def step_kernel(tp_count, m_ref, g_ref, a_ref, s_ref, first_ref, nm_ref, na_ref, ns_ref, out_ref):
    for t, pieces in enumerate(pieces_of(tp_count)):
        for start, width, into in pieces:
            cols = pl.ds(start, width)
            new_master, new_avg, new_avg_sq = step_math(
                m_ref[:, cols], g_ref[:, cols], a_ref[:, cols], s_ref[:, cols]
            )
            nm_ref[:, cols] = new_master
            na_ref[:, cols] = new_avg
            ns_ref[:, cols] = new_avg_sq
            out_ref[t, :, pl.ds(into, width)] = new_master.astype(jnp.bfloat16)


def local_step(tp_count, master, grad, exp_avg, exp_avg_sq, first):
    rows, cols = master.shape
    tile = 16
    flat = pl.BlockSpec((tile, cols), lambda i: (i, 0))
    f32 = jax.ShapeDtypeStruct((rows, cols), jnp.float32)
    return pl.pallas_call(
        functools.partial(step_kernel, tp_count),
        grid=(rows // tile,),
        in_specs=[flat] * 4 + [pl.BlockSpec(memory_space=pltpu.HBM)],
        out_specs=[flat] * 3 + [pl.BlockSpec((tp_count, tile, cols // tp_count), lambda i: (0, i, 0))],
        out_shape=[f32] * 3 + [jax.ShapeDtypeStruct((tp_count, rows, cols // tp_count), jnp.bfloat16)],
        compiler_params=pltpu.CompilerParams(vmem_limit_bytes=56 * 2**20),
        cost_estimate=pl.CostEstimate(flops=20 * rows * cols, bytes_accessed=30 * rows * cols, transcendentals=rows * cols),
    )(master, grad, exp_avg, exp_avg_sq, first)


def own_kernel(tp_count, chunks, *refs):
    sources, (out_ref, token_ref), held, sems = refs[:4], refs[4:6], refs[6:10], refs[10]
    t = lax.axis_index("tp")
    q, kv = QH // tp_count * HS, KVH // tp_count * HS
    pieces = [(t * q, q, 0), (QH * HS + t * kv, kv, q), ((QH + KVH) * HS + t * kv, kv, q + kv)]
    rows = out_ref.shape[0] // chunks
    copies = []
    for c in range(chunks):
        part = pl.ds(c * rows, rows)
        for n in range(4):
            for k, (start, width, into) in enumerate(pieces):
                copies.append(
                    pltpu.make_async_copy(
                        sources[n].at[part, pl.ds(pl.multiple_of(start, HS), width)],
                        held[n].at[part, pl.ds(into, width)],
                        sems.at[(c * 4 + n) * 3 + k],
                    )
                )
    for cp in copies:
        cp.start()
    for c in range(chunks):
        for cp in copies[c * 12 : (c + 1) * 12]:
            cp.wait()
        part = pl.ds(c * rows, rows)
        out_ref[part, :] = step_math(*[ref[part, :] for ref in held])[0].astype(jnp.bfloat16)
    token_ref[...] = jnp.zeros_like(token_ref)


def own_slice(tp_count, *arrays):
    rows, cols = arrays[0].shape
    width = cols // tp_count
    chunks = max(rows // 32, 1)
    vmem = pl.BlockSpec(memory_space=pltpu.VMEM)
    return pl.pallas_call(
        functools.partial(own_kernel, tp_count, chunks),
        in_specs=[pl.BlockSpec(memory_space=pltpu.HBM)] * 4,
        out_specs=[vmem, vmem],
        out_shape=[jax.ShapeDtypeStruct((rows, width), jnp.bfloat16), jax.ShapeDtypeStruct((8, 128), jnp.float32)],
        scratch_shapes=[pltpu.VMEM((rows, width), jnp.float32)] * 4 + [pltpu.SemaphoreType.DMA((chunks * 12,))],
        compiler_params=pltpu.CompilerParams(vmem_limit_bytes=60 * 2**20),
        cost_estimate=pl.CostEstimate(flops=20 * rows * width, bytes_accessed=18 * rows * width, transcendentals=rows * width),
    )(*arrays)


def mix(t, j, count):
    out, bit = 0, 1
    while bit < count:
        out = out + ((t // bit) % 2 + (j // bit) % 2) % 2 * bit
        bit *= 2
    return out


def spread_kernel(dp_count, tp_count, parts, own_ref, below_ref, above_ref, out_ref, own_sem, flat_send, up_send, down_send, side_send, in_recv, side_recv):
    planes = dp_count // CORES
    dp, t = lax.axis_index("dp"), lax.axis_index("tp")
    z, core = dp // CORES, dp % CORES
    rows = own_ref.shape[1]
    part_rows = rows // parts
    has_up, has_down = z < planes - 1, z > 0
    units = tp_count * parts

    up = {"dp": dp + CORES}
    down = {"dp": dp - CORES}
    side = {"dp": z * CORES + 1 - core}

    barrier = pltpu.get_barrier_semaphore()
    for j in range(1, tp_count):
        pl.semaphore_signal(barrier, inc=1, device_id={"tp": mix(t, j, tp_count)}, device_id_type=MESH)
    pl.semaphore_signal(barrier, inc=1, device_id=side, device_id_type=MESH)

    @pl.when(has_up)
    def _():
        pl.semaphore_signal(barrier, inc=1, device_id=up, device_id_type=MESH)

    @pl.when(has_down)
    def _():
        pl.semaphore_signal(barrier, inc=1, device_id=down, device_id_type=MESH)

    pl.semaphore_wait(barrier, tp_count + has_up.astype(jnp.int32) + has_down.astype(jnp.int32))

    def place(plane, which_core, unit):
        source = mix(t, unit // parts, tp_count)
        block = (plane * CORES + which_core) * tp_count + source
        start = block * rows + unit % parts * part_rows
        return out_ref.at[pl.ds(pl.multiple_of(start, part_rows), part_rows), :]

    def copy(src, dst, send, recv, target):
        return pltpu.make_async_remote_copy(
            src_ref=src, dst_ref=dst, send_sem=send, recv_sem=recv, device_id=target, device_id_type=MESH
        )

    def going_up(src, plane, unit):
        return copy(src, place(plane, core, unit), up_send.at[plane, unit], in_recv.at[plane, unit], up)

    def going_down(src, plane, unit):
        return copy(src, place(plane, core, unit), down_send.at[plane, unit], in_recv.at[plane, unit], down)

    def going_side(src, plane, unit):
        return copy(src, place(plane, core, unit), side_send.at[plane, unit], side_recv.at[plane, unit], side)

    def arrived(plane, unit):
        here = place(plane, core, unit)
        copy(here, here, side_send.at[plane, unit], in_recv.at[plane, unit], side).wait_recv()

    def own_part(which, h):
        return own_ref.at[which, pl.ds(h * part_rows, part_rows), :]

    def flat_copy(j, h):
        target = mix(t, j, tp_count)
        start = ((z * CORES + core) * tp_count + t) * rows + h * part_rows
        dst = out_ref.at[pl.ds(pl.multiple_of(start, part_rows), part_rows), :]
        unit = j * parts + h
        return copy(own_part(target, h), dst, flat_send.at[unit], in_recv.at[z, unit], {"tp": target})

    def onward(src, unit):
        @pl.when(has_up)
        def _():
            going_up(src, z, unit).start()

        @pl.when(has_down)
        def _():
            going_down(src, z, unit).start()

    def given(ref, h):
        return ref.at[pl.ds(h * part_rows, part_rows), :]

    def keep(which, src, plane, h):
        return pltpu.make_async_copy(src, place(plane, core, h), own_sem.at[which, h])

    for h in range(parts):

        @pl.when(has_up & has_down)
        def _():
            going_up(given(below_ref, h), z - 1, h).start()
            going_down(given(above_ref, h), z + 1, h).start()

        for j in range(1, tp_count):
            flat_copy(j, h).start()
    for h in range(parts):
        keep(0, own_part(t, h), z, h).start()
        going_side(own_part(t, h), z, h).start()

        @pl.when(has_down)
        def _():
            keep(1, given(below_ref, h), z - 1, h).start()
            going_side(given(below_ref, h), z - 1, h).start()

        @pl.when(has_up)
        def _():
            keep(2, given(above_ref, h), z + 1, h).start()
            going_side(given(above_ref, h), z + 1, h).start()

    @pl.loop(parts, units)
    def _(unit):
        arrived(z, unit)
        onward(place(z, core, unit), unit)
        going_side(place(z, core, unit), z, unit).start()

    @pl.loop(parts, (planes - 1) * units)
    def _(m):
        distance, unit = m // units + 1, m % units
        below, above = z - distance, z + distance

        @pl.when(below >= 0)
        def _():
            arrived(below, unit)

            @pl.when(has_up)
            def _():
                going_up(place(below, core, unit), below, unit).start()

            going_side(place(below, core, unit), below, unit).start()

        @pl.when(above < planes)
        def _():
            arrived(above, unit)

            @pl.when(has_down)
            def _():
                going_down(place(above, core, unit), above, unit).start()

            going_side(place(above, core, unit), above, unit).start()

    for h in range(parts):
        keep(0, own_part(t, h), z, h).wait()

        @pl.when(has_down)
        def _():
            keep(1, given(below_ref, h), z - 1, h).wait()

        @pl.when(has_up)
        def _():
            keep(2, given(above_ref, h), z + 1, h).wait()

    for j in range(1, tp_count):
        for h in range(parts):
            flat_copy(j, h).wait_send()

    @pl.loop(0, planes * units)
    def _(m):
        plane, unit = m // units, m % units
        here = place(plane, core, unit)
        there = place(plane, 1 - core, unit)

        early = (plane == z) & (unit < parts)

        @pl.when((plane <= z) & has_up & jnp.logical_not(early))
        def _():
            going_up(here, plane, unit).wait_send()

        @pl.when((plane >= z) & has_down & jnp.logical_not(early))
        def _():
            going_down(here, plane, unit).wait_send()

        going_side(here, plane, unit).wait_send()
        copy(there, there, side_send.at[plane, unit], side_recv.at[plane, unit], side).wait_recv()


def spread(dp_count, tp_count, own, below, above):
    rows, width = own.shape[1:]
    parts = 2 if rows % 64 == 0 else 1
    planes, units = dp_count // CORES, tp_count * parts
    grid = pltpu.SemaphoreType.DMA((planes, units))
    return pl.pallas_call(
        functools.partial(spread_kernel, dp_count, tp_count, parts),
        in_specs=[pl.BlockSpec(memory_space=pltpu.HBM)] * 3,
        out_specs=pl.BlockSpec(memory_space=pl.ANY),
        out_shape=jax.ShapeDtypeStruct((dp_count * tp_count * rows, width), jnp.bfloat16),
        scratch_shapes=[pltpu.SemaphoreType.DMA((3, parts)), pltpu.SemaphoreType.DMA((units,))] + [grid] * 5,
        compiler_params=pltpu.CompilerParams(collective_id=0, has_side_effects=True, vmem_limit_bytes=4 * 2**20),
        cost_estimate=pl.CostEstimate(flops=0, bytes_accessed=2 * dp_count * tp_count * rows * width, transcendentals=0),
    )(own, below, above)


def body(dp_count, tp_count, master, grad, exp_avg, exp_avg_sq):
    first, token = own_slice(tp_count, master, grad, exp_avg, exp_avg_sq)
    rise = [(i, i + CORES) for i in range(dp_count - CORES)]
    below = lax.ppermute(first, "dp", rise)
    above = lax.ppermute(first, "dp", [(b, a) for a, b in rise])
    new_master, new_avg, new_avg_sq, own = local_step(tp_count, master, grad, exp_avg, exp_avg_sq, token)
    return new_master, new_avg, new_avg_sq, spread(dp_count, tp_count, own, below, above)


def solution(mesh):
    flat = P(("dp", "tp"), None)
    return jax.shard_map(
        functools.partial(body, mesh.shape["dp"], mesh.shape["tp"]),
        mesh=mesh,
        in_specs=(flat,) * 4,
        out_specs=(flat, flat, flat, P(None, "tp")),
        check_vma=False,
    )
```
